32 devices in a mesh: groups: 2 (over y), sp: 4 (over z), tp: 2 (over x), dp: 2 (over core).
Axes of the slice: x: 2, y: 2, z: 4, core: 2. Of those that a mesh axis runs over, the one named last changes fastest.
Arguments:
- queries: bfloat16 [4096, 4096], P(('groups', 'tp', 'dp', 'sp')), parts along dimension 0, may hold values from -6 to 6
- keys: bfloat16 [4096, 512], P(('groups', 'tp', 'dp', 'sp')), parts along dimension 0, may hold values from -6 to 6
- values: bfloat16 [4096, 512], P(('groups', 'tp', 'dp', 'sp')), parts along dimension 0, may hold values from -6 to 6
- doc_lengths: int32 [32], P('groups'), parts along dimension 0, may hold values from 1 to 256, 2048 in all
Outputs:
- attended: bfloat16 [4096, 4096], P(('groups', 'tp', 'dp', 'sp')), parts along dimension 0
The draws below stay inside these ranges and needn't reach their ends.
There are 2 independent parts, one for each index of `groups`. The reference program is written for one: setup_inputs(seed, part) draws one part's arguments, and reference() takes and returns one part's arrays. A program takes and returns all parts, laid end to end along the dimension named above; each array names one. Nothing has to cross between parts.
Inputs may be any that keep to these rules, and one draw needn't show every extreme that they name: `doc_lengths`: 16 documents whose lengths sum to 2048; the longest has exactly 256 tokens.
All inputs are finite; a program needn't handle non-finite values.
Results may differ from the reference program's by a relative error of at most 0.0038.
Values may be sent and summed in bfloat16 or wider, within the bound.
A program may use at most 64 MiB of HBM per device.

```python
import math
import jax
import jax.numpy as jnp
import numpy as np
from jax import lax

QUERY_HEADS = 32
KEY_VALUE_HEADS = 4
HEAD_SIZE = 128
SEQUENCE_TOKENS = 2048
LONGEST_DOCUMENT = 256
NDOC = 16


def draw_keys(key, part):
    attention_output = jnp.clip(jax.random.normal(jax.random.fold_in(key, 11), (SEQUENCE_TOKENS, KEY_VALUE_HEADS * HEAD_SIZE), jnp.float32), -6.0, 6.0)
    return attention_output.astype(jnp.bfloat16)


def draw_queries(key, part):
    attention_output = jnp.clip(jax.random.normal(jax.random.fold_in(key, 13), (SEQUENCE_TOKENS, QUERY_HEADS * HEAD_SIZE), jnp.float32), -6.0, 6.0)
    return attention_output.astype(jnp.bfloat16)


def block_levels(key, shape, pieces, smallest, top_value):
    level = 1.0
    for position, parts in pieces:
        heights = jax.random.uniform(jax.random.fold_in(jax.random.fold_in(key, 6), position), (parts,), jnp.float32, smallest / len(pieces), top_value / len(pieces))
        level = level * jnp.repeat(jnp.exp(heights), shape[position] // parts).reshape((-1,) + (1,) * (len(shape) - 1 - position))
    return level


def profile(amount, total, most, slope):
    loads = [(1 << 20) // math.isqrt(grade ** slope) + 1 for grade in range(2, amount + 1)]
    rest, given = total - most - (amount - 1), [1] * (amount - 1)
    while rest > 0:
        free = [i for i in range(amount - 1) if given[i] < most]
        whole, left = sum([loads[i] for i in free]), rest
        for i in free:
            extra = min(most - given[i], max(1, left * loads[i] // whole), rest)
            given[i] = given[i] + extra
            rest = rest - extra
    return np.array([most] + given)


def uneven(key, count, total, most, slope):
    if count == 2:
        one = jax.random.randint(key, (), max(1, total - most), min(most, total - 1) + 1)
        return jnp.stack([one, total - one])
    tallies = jnp.asarray(profile(count, total, most, slope), jnp.int32)
    couples = (count - 1) // 2
    source_of, sink = tallies[1:1 + 2 * couples:2], tallies[2:2 + 2 * couples:2]
    margin = jnp.minimum(source_of - 1, most - sink)
    moved = jax.random.randint(jax.random.fold_in(key, 1), (couples,), 0, 1 << 20) % (margin + 1)
    tallies = tallies.at[1:1 + 2 * couples:2].set(source_of - moved).at[2:2 + 2 * couples:2].set(sink + moved)
    return tallies[jax.random.permutation(jax.random.fold_in(key, 2), count)]


def centred(stream_key, extent, spread, bound, shards=(), kind=jnp.bfloat16):
    array = jax.random.normal(stream_key, extent, jnp.float32) * spread
    if len(shards) > 0:
        array = block_levels(stream_key, extent, shards, -0.22, 0.18) * array
    return jnp.clip(array, min=-bound, max=bound).astype(kind)


def setup_inputs(seed: int = 0, part: int = 0) -> dict:
    key_list = jax.random.split(jax.random.key(seed), 5)
    part_splits = jax.random.split(jax.random.fold_in(key_list[4], part), 5)
    return {
        "queries": draw_queries(jax.random.fold_in(jax.random.fold_in(key_list[4], part), 71), part),
        "keys": draw_keys(jax.random.fold_in(jax.random.fold_in(key_list[4], part), 71), part),
        "values": centred(part_splits[2], (SEQUENCE_TOKENS, KEY_VALUE_HEADS * HEAD_SIZE), 1.0, 6.0, ((0, 16),)),
        "doc_lengths": uneven(part_splits[3], NDOC, SEQUENCE_TOKENS, LONGEST_DOCUMENT, 2).astype(jnp.int32),
    }


def reference(queries, keys, values, doc_lengths):
    ends = jnp.cumsum(doc_lengths).astype(jnp.int32)
    positions = jnp.arange(SEQUENCE_TOKENS, dtype=jnp.int32)
    doc = jnp.sum((positions[:, None] >= ends[None, :]).astype(jnp.int32), axis=1)
    query_group = QUERY_HEADS // KEY_VALUE_HEADS
    block = math.gcd(LONGEST_DOCUMENT, 512)
    blocks = SEQUENCE_TOKENS // block
    reach = LONGEST_DOCUMENT + block
    q_heads = queries.reshape(SEQUENCE_TOKENS, QUERY_HEADS, HEAD_SIZE).transpose(1, 0, 2)
    leading_part = jnp.zeros((LONGEST_DOCUMENT, KEY_VALUE_HEADS * HEAD_SIZE), jnp.bfloat16)
    key_head_rows = jnp.concatenate([leading_part, keys], axis=0).reshape(SEQUENCE_TOKENS + LONGEST_DOCUMENT, KEY_VALUE_HEADS, HEAD_SIZE).transpose(1, 0, 2)
    value_head_rows = jnp.concatenate([leading_part, values], axis=0).reshape(SEQUENCE_TOKENS + LONGEST_DOCUMENT, KEY_VALUE_HEADS, HEAD_SIZE).transpose(1, 0, 2)
    pad_pos = jnp.arange(SEQUENCE_TOKENS + LONGEST_DOCUMENT, dtype=jnp.int32) - LONGEST_DOCUMENT
    pad_doc = jnp.concatenate([jnp.full((LONGEST_DOCUMENT,), -1, jnp.int32), doc.astype(jnp.int32)], axis=0)
    scale = HEAD_SIZE ** -0.5

    def one_head(head):
        q_all = lax.dynamic_index_in_dim(q_heads, head, 0, keepdims=False)
        k_all = lax.dynamic_index_in_dim(key_head_rows, head // query_group, 0, keepdims=False)
        v_all = lax.dynamic_index_in_dim(value_head_rows, head // query_group, 0, keepdims=False)

        def one_block(index):
            first = (index * block).astype(jnp.int32)
            q_rows = lax.dynamic_slice_in_dim(q_all, first, block, 0)
            q_pos = first + jnp.arange(block, dtype=jnp.int32)
            q_doc = lax.dynamic_slice_in_dim(doc, first, block, 0)
            k_rows = lax.dynamic_slice_in_dim(k_all, first, reach, 0)
            v_rows = lax.dynamic_slice_in_dim(v_all, first, reach, 0)
            k_pos = lax.dynamic_slice_in_dim(pad_pos, first, reach, 0)
            k_doc = lax.dynamic_slice_in_dim(pad_doc, first, reach, 0)
            score = jnp.dot(q_rows, k_rows.T, preferred_element_type=jnp.float32) * scale
            live = (k_pos[None, :] <= q_pos[:, None]) & (k_doc[None, :] == q_doc[:, None])
            top = jnp.max(jnp.where(live, score, -jnp.inf), axis=1)
            weight = jnp.where(live, jnp.exp(score - top[:, None]), 0.0)
            total = jnp.sum(weight, axis=1)
            summed = jnp.dot(weight.astype(jnp.bfloat16), v_rows, preferred_element_type=jnp.float32)
            return (summed / total[:, None]).astype(jnp.bfloat16)

        return lax.map(one_block, jnp.arange(blocks, dtype=jnp.int32)).reshape(SEQUENCE_TOKENS, HEAD_SIZE)

    attention_output = lax.map(one_head, jnp.arange(QUERY_HEADS, dtype=jnp.int32))
    return attention_output.transpose(1, 0, 2).reshape(SEQUENCE_TOKENS, QUERY_HEADS * HEAD_SIZE)
```

```python
import functools
import math

import jax
import jax.numpy as jnp
from jax import lax
from jax.experimental import pallas as pl
from jax.experimental.pallas import tpu as pltpu
from jax.sharding import PartitionSpec as P

HEAD_SIZE = 128
MESH = pl.DeviceIdType.MESH
DEAD = -1e30


def place(index, dp_count, sp_count):
    return {
        "tp": index // (dp_count * sp_count),
        "dp": (index // sp_count) % dp_count,
        "sp": index % sp_count,
    }


def kernel(
    sizes, q_hbm, k_hbm, v_hbm, lengths, out_hbm,
    q_buf, held, bias, out_buf, q_sem, kv_sem, send_sem, recv_sem, out_sem,
):
    tp_count, dp_count, sp_count, hops, heads, group = sizes
    rows = q_hbm.shape[0]
    width = group * HEAD_SIZE
    blocks = tp_count * dp_count * sp_count
    me = (lax.axis_index("tp") * dp_count + lax.axis_index("dp")) * sp_count + lax.axis_index("sp")
    right = place(lax.rem(me + 1, blocks), dp_count, sp_count)
    left = place(lax.rem(me + blocks - 1, blocks), dp_count, sp_count)

    def load(source, which, head):
        columns = pl.ds(head * HEAD_SIZE, HEAD_SIZE)
        return pltpu.make_async_copy(
            source.at[:, columns], held.at[0, head, which], kv_sem.at[head, which]
        )

    def load_q(head):
        columns = pl.ds(head * width, width)
        return pltpu.make_async_copy(q_hbm.at[:, columns], q_buf.at[:, columns], q_sem.at[head])

    def store(head):
        columns = pl.ds(head * width, width)
        return pltpu.make_async_copy(out_buf.at[:, columns], out_hbm.at[:, columns], out_sem.at[head])

    def send(hop, head):
        return pltpu.make_async_remote_copy(
            src_ref=held.at[hop, head],
            dst_ref=held.at[hop + 1, head],
            send_sem=send_sem.at[hop, head],
            recv_sem=recv_sem.at[hop, head],
            device_id=right,
            device_id_type=MESH,
        )

    for head in range(heads):
        load(k_hbm, 0, head).start()
        load(v_hbm, 1, head).start()
    for head in range(heads):
        load_q(head).start()

    barrier = pltpu.get_barrier_semaphore()
    for neighbour in (left, right):
        pl.semaphore_signal(barrier, inc=1, device_id=neighbour, device_id_type=MESH)
    pl.semaphore_wait(barrier, 2)

    for head in range(heads):
        load(k_hbm, 0, head).wait()
        load(v_hbm, 1, head).wait()
        send(0, head).start()

    base = me * rows
    position = base + lax.broadcasted_iota(jnp.int32, (rows, rows), 0)
    column = lax.broadcasted_iota(jnp.int32, (rows, rows), 1)
    first = jnp.zeros((rows, rows), jnp.int32)
    end = jnp.int32(0)
    for entry in range(lengths.shape[0]):
        end = end + lengths[entry]
        first = jnp.where(position >= end, end, first)
    for hop in range(hops + 1):
        key_position = base - hop * rows + column
        live = (key_position >= first) & (key_position <= position)
        bias[:, hop * rows : (hop + 1) * rows] = jnp.where(live, 0.0, DEAD)

    for hop in range(1, hops):
        for head in range(heads):
            send(hop - 1, head).wait_recv()
            send(hop, head).start()

    factor = HEAD_SIZE ** (-0.5) * math.log2(math.e)
    span = (hops + 1) * rows
    for head in range(heads):
        send(hops - 1, head).wait_recv()
        load_q(head).wait()
        k_all = held[:, head, 0].reshape(span, HEAD_SIZE)
        v_all = held[:, head, 1].reshape(span, HEAD_SIZE)
        for member in range(group):
            place_at = head * width + member * HEAD_SIZE
            q_rows = q_buf[:, place_at : place_at + HEAD_SIZE]
            score = lax.dot_general(
                q_rows, k_all, (((1,), (1,)), ((), ())), preferred_element_type=jnp.float32
            ) + bias[...]
            top = jnp.max(score, axis=1, keepdims=True)
            weight = jnp.exp2((score - top) * factor)
            total = jnp.sum(weight, axis=1, keepdims=True)
            summed = jnp.dot(weight.astype(jnp.bfloat16), v_all, preferred_element_type=jnp.float32)
            out_buf[:, place_at : place_at + HEAD_SIZE] = (summed / total).astype(jnp.bfloat16)
        store(head).start()

    for hop in range(hops):
        for head in range(heads):
            send(hop, head).wait_send()
    for head in range(heads):
        store(head).wait()


def solution(mesh):
    tp_count, dp_count, sp_count = (mesh.shape[axis] for axis in ("tp", "dp", "sp"))
    hops = max(sp_count // 2, 1)

    def local(queries, keys, values, doc_lengths):
        rows, width = queries.shape
        heads = keys.shape[1] // HEAD_SIZE
        group = width // keys.shape[1]
        sizes = (tp_count, dp_count, sp_count, hops, heads, group)
        hbm = pl.BlockSpec(memory_space=pl.ANY)
        return pl.pallas_call(
            functools.partial(kernel, sizes),
            out_shape=jax.ShapeDtypeStruct((rows, width), jnp.bfloat16),
            in_specs=[hbm, hbm, hbm, pl.BlockSpec(memory_space=pltpu.SMEM)],
            out_specs=hbm,
            scratch_shapes=[
                pltpu.VMEM((rows, width), jnp.bfloat16),
                pltpu.VMEM((hops + 1, heads, 2, rows, HEAD_SIZE), jnp.bfloat16),
                pltpu.VMEM((rows, (hops + 1) * rows), jnp.float32),
                pltpu.VMEM((rows, width), jnp.bfloat16),
                pltpu.SemaphoreType.DMA((heads,)),
                pltpu.SemaphoreType.DMA((heads, 2)),
                pltpu.SemaphoreType.DMA((hops, heads)),
                pltpu.SemaphoreType.DMA((hops, heads)),
                pltpu.SemaphoreType.DMA((heads,)),
            ],
            compiler_params=pltpu.CompilerParams(collective_id=0, has_side_effects=True),
        )(queries, keys, values, doc_lengths)

    spec = P(("groups", "tp", "dp", "sp"), None)
    return jax.shard_map(
        local, mesh=mesh, in_specs=(spec, spec, spec, P("groups")), out_specs=spec, check_vma=False
    )
```

```python
import functools
import math

import jax
import jax.numpy as jnp
from jax import lax
from jax.experimental import pallas as pl
from jax.experimental.pallas import tpu as pltpu
from jax.sharding import PartitionSpec as P

HEAD_SIZE = 128
MESH = pl.DeviceIdType.MESH
DEAD = -1e30


def place(index, dp_count, sp_count):
    return {
        "tp": index // (dp_count * sp_count),
        "dp": (index // sp_count) % dp_count,
        "sp": index % sp_count,
    }


def kernel(
    sizes, q_hbm, k_hbm, v_hbm, lengths, out_hbm,
    q_buf, held, bias, out_buf, q_sem, kv_sem, send_sem, recv_sem, out_sem,
):
    tp_count, dp_count, sp_count, hops, heads, group = sizes
    rows = q_hbm.shape[0]
    width = group * HEAD_SIZE
    blocks = tp_count * dp_count * sp_count
    me = (lax.axis_index("tp") * dp_count + lax.axis_index("dp")) * sp_count + lax.axis_index("sp")
    right = place(lax.rem(me + 1, blocks), dp_count, sp_count)
    left = place(lax.rem(me + blocks - 1, blocks), dp_count, sp_count)

    def load(source, which, head):
        columns = pl.ds(head * HEAD_SIZE, HEAD_SIZE)
        return pltpu.make_async_copy(
            source.at[:, columns], held.at[0, head, which], kv_sem.at[head, which]
        )

    def load_q(head):
        columns = pl.ds(head * width, width)
        return pltpu.make_async_copy(q_hbm.at[:, columns], q_buf.at[:, columns], q_sem.at[head])

    def store(head):
        columns = pl.ds(head * width, width)
        return pltpu.make_async_copy(out_buf.at[:, columns], out_hbm.at[:, columns], out_sem.at[head])

    def send(hop, head):
        return pltpu.make_async_remote_copy(
            src_ref=held.at[hop, head],
            dst_ref=held.at[hop + 1, head],
            send_sem=send_sem.at[hop, head],
            recv_sem=recv_sem.at[hop, head],
            device_id=right,
            device_id_type=MESH,
        )

    for head in range(heads):
        load(k_hbm, 0, head).start()
        load(v_hbm, 1, head).start()
    for head in range(heads):
        load_q(head).start()

    barrier = pltpu.get_barrier_semaphore()
    for neighbour in (left, right):
        pl.semaphore_signal(barrier, inc=1, device_id=neighbour, device_id_type=MESH)
    pl.semaphore_wait(barrier, 2)

    for head in range(heads):
        load(k_hbm, 0, head).wait()
        load(v_hbm, 1, head).wait()
        send(0, head).start()

    base = me * rows
    row = lax.broadcasted_iota(jnp.int32, (rows, rows), 0)
    column = lax.broadcasted_iota(jnp.int32, (rows, rows), 1)
    near = column <= row
    first = jnp.zeros((rows, rows), jnp.int32)
    end = jnp.int32(0)
    for entry in range(lengths.shape[0]):
        end = end + lengths[entry]
        first = jnp.where(base + row >= end, end, first)
    mixed_position = base + column - jnp.where(near, 0, hops * rows)
    bias[0] = jnp.where(mixed_position >= first, 0.0, DEAD)
    for hop in range(1, hops):
        bias[hop] = jnp.where(base - hop * rows + column >= first, 0.0, DEAD)

    for hop in range(1, hops):
        for head in range(heads):
            send(hop - 1, head).wait_recv()
            send(hop, head).start()

    factor = HEAD_SIZE ** (-0.5) * math.log2(math.e)
    span = (hops + 1) * rows
    batch = math.gcd(group, 8)
    for head in range(heads):
        send(hops - 1, head).wait_recv()
        load_q(head).wait()
        k_all = held[:, head, 0].reshape(span, HEAD_SIZE)
        v_all = held[:, head, 1].reshape(span, HEAD_SIZE)
        for member in range(0, group, batch):
            at = [head * width + (member + other) * HEAD_SIZE for other in range(batch)]
            q_rows = jnp.concatenate([q_buf[:, a : a + HEAD_SIZE] for a in at], axis=0)
            score = lax.dot_general(
                q_rows, k_all, (((1,), (1,)), ((), ())), preferred_element_type=jnp.float32
            ).reshape(batch, rows, span)
            parts = [score[:, :, hop * rows : (hop + 1) * rows] for hop in range(hops + 1)]
            mixed = jnp.where(near, parts[0], parts[hops])
            parts = [part + bias[hop] for hop, part in enumerate([mixed] + parts[1:hops])]
            top = jnp.max(functools.reduce(jnp.maximum, parts), axis=2, keepdims=True)
            weights = [jnp.exp2((part - top) * factor) for part in parts]
            total = jnp.sum(sum(weights[1:], weights[0]), axis=2, keepdims=True)
            ends = [jnp.where(near, weights[0], 0.0), jnp.where(near, 0.0, weights[0])]
            weight = jnp.concatenate([ends[0]] + weights[1:] + [ends[1]], axis=2)
            weight = weight.astype(jnp.bfloat16).reshape(batch * rows, span)
            summed = jnp.dot(weight, v_all, preferred_element_type=jnp.float32)
            result = (summed.reshape(batch, rows, HEAD_SIZE) / total).astype(jnp.bfloat16)
            for other, a in enumerate(at):
                out_buf[:, a : a + HEAD_SIZE] = result[other]
        store(head).start()

    for hop in range(hops):
        for head in range(heads):
            send(hop, head).wait_send()
    for head in range(heads):
        store(head).wait()


def solution(mesh):
    tp_count, dp_count, sp_count = (mesh.shape[axis] for axis in ("tp", "dp", "sp"))
    hops = max(sp_count // 2, 1)

    def local(queries, keys, values, doc_lengths):
        rows, width = queries.shape
        heads = keys.shape[1] // HEAD_SIZE
        group = width // keys.shape[1]
        sizes = (tp_count, dp_count, sp_count, hops, heads, group)
        hbm = pl.BlockSpec(memory_space=pl.ANY)
        return pl.pallas_call(
            functools.partial(kernel, sizes),
            out_shape=jax.ShapeDtypeStruct((rows, width), jnp.bfloat16),
            in_specs=[hbm, hbm, hbm, pl.BlockSpec(memory_space=pltpu.SMEM)],
            out_specs=hbm,
            scratch_shapes=[
                pltpu.VMEM((rows, width), jnp.bfloat16),
                pltpu.VMEM((hops + 1, heads, 2, rows, HEAD_SIZE), jnp.bfloat16),
                pltpu.VMEM((hops, rows, rows), jnp.float32),
                pltpu.VMEM((rows, width), jnp.bfloat16),
                pltpu.SemaphoreType.DMA((heads,)),
                pltpu.SemaphoreType.DMA((heads, 2)),
                pltpu.SemaphoreType.DMA((hops, heads)),
                pltpu.SemaphoreType.DMA((hops, heads)),
                pltpu.SemaphoreType.DMA((heads,)),
            ],
            compiler_params=pltpu.CompilerParams(collective_id=0, has_side_effects=True),
        )(queries, keys, values, doc_lengths)

    spec = P(("groups", "tp", "dp", "sp"), None)
    return jax.shard_map(
        local, mesh=mesh, in_specs=(spec, spec, spec, P("groups")), out_specs=spec, check_vma=False
    )
```

```python
import functools
import math

import jax
import jax.numpy as jnp
from jax import lax
from jax.experimental import pallas as pl
from jax.experimental.pallas import tpu as pltpu
from jax.sharding import PartitionSpec as P

HEAD_SIZE = 128
MESH = pl.DeviceIdType.MESH
DEAD = -1e30


def place(index, dp_count, sp_count):
    return {
        "tp": index // (dp_count * sp_count),
        "dp": (index // sp_count) % dp_count,
        "sp": index % sp_count,
    }


def kernel(
    sizes, q_hbm, k_hbm, v_hbm, lengths_hbm, out_buf,
    q_buf, held, bias, lengths, q_sem, kv_sem, send_sem, recv_sem, lengths_sem,
):
    tp_count, dp_count, sp_count, hops, heads, group = sizes
    rows = q_hbm.shape[0]
    width = group * HEAD_SIZE
    blocks = tp_count * dp_count * sp_count
    me = (lax.axis_index("tp") * dp_count + lax.axis_index("dp")) * sp_count + lax.axis_index("sp")
    right = place(lax.rem(me + 1, blocks), dp_count, sp_count)
    left = place(lax.rem(me + blocks - 1, blocks), dp_count, sp_count)

    def load(source, which, head):
        columns = pl.ds(head * HEAD_SIZE, HEAD_SIZE)
        return pltpu.make_async_copy(
            source.at[:, columns], held.at[0, head, which], kv_sem.at[head, which]
        )

    def load_q(head):
        columns = pl.ds(head * width, width)
        return pltpu.make_async_copy(q_hbm.at[:, columns], q_buf.at[:, columns], q_sem.at[head])

    def send(hop, head):
        return pltpu.make_async_remote_copy(
            src_ref=held.at[hop, head],
            dst_ref=held.at[hop + 1, head],
            send_sem=send_sem.at[hop, head],
            recv_sem=recv_sem.at[hop, head],
            device_id=right,
            device_id_type=MESH,
        )

    def start_send(hop, head):
        @pl.when((me >= hop) & (me < blocks - 1))
        def _():
            send(hop, head).start()

    def wait_receive(hop, head):
        @pl.when(me >= hop)
        def _():
            send(hop - 1, head).wait_recv()

    get_lengths = pltpu.make_async_copy(lengths_hbm, lengths, lengths_sem)
    for head in range(heads):
        load(k_hbm, 0, head).start()
        load(v_hbm, 1, head).start()
    for head in range(heads):
        load_q(head).start()
    get_lengths.start()

    barrier = pltpu.get_barrier_semaphore()

    @pl.when(me > 0)
    def _():
        pl.semaphore_signal(barrier, inc=1, device_id=left, device_id_type=MESH)

    @pl.when(me < blocks - 1)
    def _():
        pl.semaphore_wait(barrier, 1)

    for head in range(heads):
        load(k_hbm, 0, head).wait()
        load(v_hbm, 1, head).wait()
        start_send(0, head)
    for hop in range(1, hops + 1):

        @pl.when(me < hop)
        def _():
            held[hop] = jnp.zeros_like(held[hop])

    get_lengths.wait()
    base = me * rows
    row = lax.broadcasted_iota(jnp.int32, (rows, rows), 0)
    column = lax.broadcasted_iota(jnp.int32, (rows, rows), 1)
    near = column <= row
    first = jnp.zeros((rows, rows), jnp.int32)
    end = jnp.int32(0)
    for entry in range(lengths.shape[0]):
        end = end + lengths[entry]
        first = jnp.where(base + row >= end, end, first)
    mixed_position = base + column - jnp.where(near, 0, hops * rows)
    bias[0] = jnp.where(mixed_position >= first, 0.0, DEAD)
    for hop in range(1, hops):
        bias[hop] = jnp.where(base - hop * rows + column >= first, 0.0, DEAD)

    for hop in range(1, hops):
        for head in range(heads):
            wait_receive(hop, head)
            start_send(hop, head)

    factor = HEAD_SIZE ** (-0.5) * math.log2(math.e)
    span = (hops + 1) * rows
    batch = math.gcd(group, 8)
    for head in range(heads):
        wait_receive(hops, head)
        load_q(head).wait()
        k_all = held[:, head, 0].reshape(span, HEAD_SIZE)
        v_all = held[:, head, 1].reshape(span, HEAD_SIZE)
        for member in range(0, group, batch):
            at = [head * width + (member + other) * HEAD_SIZE for other in range(batch)]
            q_rows = jnp.concatenate([q_buf[:, a : a + HEAD_SIZE] for a in at], axis=0)
            score = lax.dot_general(
                q_rows, k_all, (((1,), (1,)), ((), ())), preferred_element_type=jnp.float32
            ).reshape(batch, rows, span)
            parts = [score[:, :, hop * rows : (hop + 1) * rows] for hop in range(hops + 1)]
            mixed = jnp.where(near, parts[0], parts[hops])
            parts = [part + bias[hop] for hop, part in enumerate([mixed] + parts[1:hops])]
            top = jnp.max(functools.reduce(jnp.maximum, parts), axis=2, keepdims=True)
            weights = [jnp.exp2((part - top) * factor) for part in parts]
            total = jnp.sum(sum(weights[1:], weights[0]), axis=2, keepdims=True)
            ends = [jnp.where(near, weights[0], 0.0), jnp.where(near, 0.0, weights[0])]
            weight = jnp.concatenate([ends[0]] + weights[1:] + [ends[1]], axis=2)
            weight = weight.astype(jnp.bfloat16).reshape(batch * rows, span)
            summed = jnp.dot(weight, v_all, preferred_element_type=jnp.float32)
            result = (summed.reshape(batch, rows, HEAD_SIZE) / total).astype(jnp.bfloat16)
            for other, a in enumerate(at):
                out_buf[:, a : a + HEAD_SIZE] = result[other]

    for hop in range(hops):
        for head in range(heads):

            @pl.when((me >= hop) & (me < blocks - 1))
            def _():
                send(hop, head).wait_send()


def solution(mesh):
    tp_count, dp_count, sp_count = (mesh.shape[axis] for axis in ("tp", "dp", "sp"))
    hops = max(sp_count // 2, 1)

    def local(queries, keys, values, doc_lengths):
        rows, width = queries.shape
        heads = keys.shape[1] // HEAD_SIZE
        group = width // keys.shape[1]
        sizes = (tp_count, dp_count, sp_count, hops, heads, group)
        hbm = pl.BlockSpec(memory_space=pltpu.HBM)
        return pl.pallas_call(
            functools.partial(kernel, sizes),
            out_shape=jax.ShapeDtypeStruct((rows, width), jnp.bfloat16),
            in_specs=[hbm, hbm, hbm, hbm],
            out_specs=pl.BlockSpec(memory_space=pltpu.VMEM),
            scratch_shapes=[
                pltpu.VMEM((rows, width), jnp.bfloat16),
                pltpu.VMEM((hops + 1, heads, 2, rows, HEAD_SIZE), jnp.bfloat16),
                pltpu.VMEM((hops, rows, rows), jnp.float32),
                pltpu.SMEM(doc_lengths.shape, jnp.int32),
                pltpu.SemaphoreType.DMA((heads,)),
                pltpu.SemaphoreType.DMA((heads, 2)),
                pltpu.SemaphoreType.DMA((hops, heads)),
                pltpu.SemaphoreType.DMA((hops, heads)),
                pltpu.SemaphoreType.DMA,
            ],
            compiler_params=pltpu.CompilerParams(collective_id=0, has_side_effects=True, vmem_limit_bytes=32 << 20),
        )(queries, keys, values, doc_lengths)

    spec = P(("groups", "tp", "dp", "sp"), None)
    return jax.shard_map(
        local, mesh=mesh, in_specs=(spec, spec, spec, P("groups")), out_specs=spec, check_vma=False
    )
```

```python
import functools
import math

import jax
import jax.numpy as jnp
from jax import lax
from jax.experimental import pallas as pl
from jax.experimental.pallas import tpu as pltpu
from jax.sharding import PartitionSpec as P

HEAD_SIZE = 128
MESH = pl.DeviceIdType.MESH
DEAD = -1e30


def place(index, dp_count, sp_count):
    return {
        "tp": index // (dp_count * sp_count),
        "dp": (index // sp_count) % dp_count,
        "sp": index % sp_count,
    }


def kernel(
    sizes, q_hbm, k_hbm, v_hbm, lengths_hbm, out_buf,
    q_buf, held, bias, lengths, q_sem, kv_sem, send_sem, recv_sem, lengths_sem, across_sem, carried, lent_sem, carried_sem,
):
    tp_count, dp_count, sp_count, hops, heads, group = sizes
    rows = q_hbm.shape[0]
    width = group * HEAD_SIZE
    blocks = tp_count * dp_count * sp_count
    tp, dp, position = (lax.axis_index(axis) for axis in ("tp", "dp", "sp"))
    me = (tp * dp_count + dp) * sp_count + position
    right = place(lax.rem(me + 1, blocks), dp_count, sp_count)
    left = place(lax.rem(me + blocks - 1, blocks), dp_count, sp_count)

    def load(source, which, head):
        columns = pl.ds(head * HEAD_SIZE, HEAD_SIZE)
        return pltpu.make_async_copy(
            source.at[:, columns], held.at[0, head, which], kv_sem.at[head, which]
        )

    def load_q(head):
        columns = pl.ds(head * width, width)
        return pltpu.make_async_copy(q_hbm.at[:, columns], q_buf.at[:, columns], q_sem.at[head])

    def send(hop, head):
        return pltpu.make_async_remote_copy(
            src_ref=held.at[hop, head],
            dst_ref=held.at[hop + 1, head],
            send_sem=send_sem.at[hop, head],
            recv_sem=recv_sem.at[hop, head],
            device_id=right,
            device_id_type=MESH,
        )

    ahead = sp_count - position
    crosses = (ahead <= hops) & (me + ahead < blocks)
    across = place(jnp.minimum(me + ahead, blocks - 1), dp_count, sp_count)
    edge = (dp == dp_count - 1) & (ahead <= hops)
    lends = edge & (tp == tp_count - 2)
    carries = edge & (tp == tp_count - 1) & (tp_count > 1)
    lent = heads // 2
    carrier = {"tp": jnp.minimum(tp + 1, tp_count - 1), "dp": dp, "sp": position}
    lender = {"tp": jnp.maximum(tp - 1, 0), "dp": dp, "sp": position}
    goal = {"tp": tp, "dp": 0, "sp": 0}

    def sends(hop):
        return (me >= hop) & (position < sp_count - 1)

    def start_send(hop, head):
        @pl.when(sends(hop))
        def _():
            send(hop, head).start()

    def wait_receive(hop, head):
        @pl.when(me >= hop)
        def _():
            send(hop - 1, head).wait_recv()

    def send_across(source, sem, target, distance, head):
        return pltpu.make_async_remote_copy(
            src_ref=source.at[head],
            dst_ref=held.at[distance, head],
            send_sem=sem.at[head],
            recv_sem=recv_sem.at[distance - 1, head],
            device_id=target,
            device_id_type=MESH,
        )

    def lend(head):
        return pltpu.make_async_remote_copy(
            src_ref=held.at[0, head],
            dst_ref=carried.at[head],
            send_sem=across_sem.at[head],
            recv_sem=lent_sem.at[head],
            device_id=carrier,
            device_id_type=MESH,
        )

    def each_lent(action):
        @pl.when(lends)
        def _():
            for head in range(lent):
                action(lend(head))

    def each_across(action):
        for distance in range(1, hops + 1):

            @pl.when(crosses & (ahead == distance))
            def _():
                @pl.when(jnp.logical_not(lends))
                def _():
                    for head in range(lent):
                        action(send_across(held.at[0], across_sem, across, distance, head))

                for head in range(lent, heads):
                    action(send_across(held.at[0], across_sem, across, distance, head))

    def each_carried(action):
        for distance in range(1, hops + 1):

            @pl.when(carries & (ahead == distance))
            def _():
                for head in range(lent):
                    action(head, send_across(carried, carried_sem, goal, distance, head))

    def forward(head, copy):
        lend(head).wait_recv()
        copy.start()

    get_lengths = pltpu.make_async_copy(lengths_hbm, lengths, lengths_sem)
    for head in range(heads):
        load(k_hbm, 0, head).start()
        load(v_hbm, 1, head).start()
    for head in range(heads):
        load_q(head).start()
    get_lengths.start()

    barrier = pltpu.get_barrier_semaphore()

    def greet(device):
        pl.semaphore_signal(barrier, inc=1, device_id=device, device_id_type=MESH)

    @pl.when(position > 0)
    def _():
        greet(left)

    for distance in range(1, hops + 1):

        @pl.when((position == 0) & (me >= distance))
        def _():
            greet(place(jnp.maximum(me - distance, 0), dp_count, sp_count))

        @pl.when((position == 0) & (dp == 0) & (tp == tp_count - 1) & (tp_count > 1))
        def _():
            greet({"tp": tp, "dp": dp_count - 1, "sp": sp_count - distance})

    @pl.when(carries)
    def _():
        greet(lender)

    peers = [position < sp_count - 1, crosses, lends, carries]
    count = sum(peer.astype(jnp.int32) for peer in peers)
    for number in range(1, len(peers) + 1):

        @pl.when(count == number)
        def _():
            pl.semaphore_wait(barrier, number)

    for head in range(heads):
        load(k_hbm, 0, head).wait()
        load(v_hbm, 1, head).wait()
        start_send(0, head)
    each_lent(lambda copy: copy.start())
    each_across(lambda copy: copy.start())
    each_carried(forward)
    for hop in range(1, hops + 1):

        @pl.when(me < hop)
        def _():
            held[hop] = jnp.zeros_like(held[hop])

    get_lengths.wait()
    base = me * rows
    row = lax.broadcasted_iota(jnp.int32, (rows, rows), 0)
    column = lax.broadcasted_iota(jnp.int32, (rows, rows), 1)
    near = column <= row
    first = jnp.zeros((rows, rows), jnp.int32)
    end = jnp.int32(0)
    for entry in range(lengths.shape[0]):
        end = end + lengths[entry]
        first = jnp.where(base + row >= end, end, first)
    mixed_position = base + column - jnp.where(near, 0, hops * rows)
    bias[0] = jnp.where(mixed_position >= first, 0.0, DEAD)
    for hop in range(1, hops):
        bias[hop] = jnp.where(base - hop * rows + column >= first, 0.0, DEAD)

    for hop in range(1, hops):
        for head in range(heads):
            wait_receive(hop, head)
            start_send(hop, head)

    factor = HEAD_SIZE ** (-0.5) * math.log2(math.e)
    span = (hops + 1) * rows
    batch = math.gcd(group, 8)
    for head in range(heads):
        wait_receive(hops, head)
        load_q(head).wait()
        k_all = held[:, head, 0].reshape(span, HEAD_SIZE)
        v_all = held[:, head, 1].reshape(span, HEAD_SIZE)
        for member in range(0, group, batch):
            at = [head * width + (member + other) * HEAD_SIZE for other in range(batch)]
            q_rows = jnp.concatenate([q_buf[:, a : a + HEAD_SIZE] for a in at], axis=0)
            score = lax.dot_general(
                q_rows, k_all, (((1,), (1,)), ((), ())), preferred_element_type=jnp.float32
            ).reshape(batch, rows, span)
            parts = [score[:, :, hop * rows : (hop + 1) * rows] for hop in range(hops + 1)]
            mixed = jnp.where(near, parts[0], parts[hops])
            parts = [part + bias[hop] for hop, part in enumerate([mixed] + parts[1:hops])]
            top = jnp.max(functools.reduce(jnp.maximum, parts), axis=2, keepdims=True)
            weights = [jnp.exp2((part - top) * factor) for part in parts]
            total = jnp.sum(sum(weights[1:], weights[0]), axis=2, keepdims=True)
            ends = [jnp.where(near, weights[0], 0.0), jnp.where(near, 0.0, weights[0])]
            weight = jnp.concatenate([ends[0]] + weights[1:] + [ends[1]], axis=2)
            weight = weight.astype(jnp.bfloat16).reshape(batch * rows, span)
            summed = jnp.dot(weight, v_all, preferred_element_type=jnp.float32)
            result = (summed.reshape(batch, rows, HEAD_SIZE) / total).astype(jnp.bfloat16)
            for other, a in enumerate(at):
                out_buf[:, a : a + HEAD_SIZE] = result[other]

    for hop in range(hops):
        for head in range(heads):

            @pl.when(sends(hop))
            def _():
                send(hop, head).wait_send()
    each_lent(lambda copy: copy.wait_send())
    each_across(lambda copy: copy.wait_send())
    each_carried(lambda head, copy: copy.wait_send())


def solution(mesh):
    tp_count, dp_count, sp_count = (mesh.shape[axis] for axis in ("tp", "dp", "sp"))
    hops = max(sp_count // 2, 1)

    def local(queries, keys, values, doc_lengths):
        rows, width = queries.shape
        heads = keys.shape[1] // HEAD_SIZE
        group = width // keys.shape[1]
        sizes = (tp_count, dp_count, sp_count, hops, heads, group)
        hbm = pl.BlockSpec(memory_space=pltpu.HBM)
        return pl.pallas_call(
            functools.partial(kernel, sizes),
            out_shape=pltpu.VMEM((rows, width), jnp.bfloat16),
            in_specs=[hbm, hbm, hbm, hbm],
            out_specs=pl.BlockSpec(memory_space=pltpu.VMEM),
            scratch_shapes=[
                pltpu.VMEM((rows, width), jnp.bfloat16),
                pltpu.VMEM((hops + 1, heads, 2, rows, HEAD_SIZE), jnp.bfloat16),
                pltpu.VMEM((hops, rows, rows), jnp.float32),
                pltpu.SMEM(doc_lengths.shape, jnp.int32),
                pltpu.SemaphoreType.DMA((heads,)),
                pltpu.SemaphoreType.DMA((heads, 2)),
                pltpu.SemaphoreType.DMA((hops, heads)),
                pltpu.SemaphoreType.DMA((hops, heads)),
                pltpu.SemaphoreType.DMA,
                pltpu.SemaphoreType.DMA((heads,)),
                pltpu.VMEM((max(heads // 2, 1), 2, rows, HEAD_SIZE), jnp.bfloat16),
                pltpu.SemaphoreType.DMA((heads,)),
                pltpu.SemaphoreType.DMA((heads,)),
            ],
            compiler_params=pltpu.CompilerParams(collective_id=0, has_side_effects=True, vmem_limit_bytes=32 << 20),
        )(*(pltpu.with_memory_space_constraint(a, pltpu.HBM) for a in (queries, keys, values, doc_lengths)))

    spec = P(("groups", "tp", "dp", "sp"), None)
    return jax.shard_map(
        local, mesh=mesh, in_specs=(spec, spec, spec, P("groups")), out_specs=spec, check_vma=False
    )
```

```python
import functools
import math

import jax
import jax.numpy as jnp
from jax import lax
from jax.experimental import pallas as pl
from jax.experimental.pallas import tpu as pltpu
from jax.sharding import PartitionSpec as P

HEAD_SIZE = 128
MESH = pl.DeviceIdType.MESH
DEAD = -1e30


def place(index, dp_count, sp_count):
    return {
        "tp": index // (dp_count * sp_count),
        "dp": (index // sp_count) % dp_count,
        "sp": index % sp_count,
    }


def kernel(
    sizes, q_hbm, k_hbm, v_hbm, lengths_hbm, out_buf,
    q_buf, held, bias, lengths, q_sem, kv_sem, send_sem, recv_sem, lengths_sem, across_sem, carried, lent_sem, carried_sem,
):
    tp_count, dp_count, sp_count, hops, heads, group = sizes
    rows = q_hbm.shape[0]
    width = group * HEAD_SIZE
    blocks = tp_count * dp_count * sp_count
    tp, dp, position = (lax.axis_index(axis) for axis in ("tp", "dp", "sp"))
    me = (tp * dp_count + dp) * sp_count + position
    right = place(lax.rem(me + 1, blocks), dp_count, sp_count)
    left = place(lax.rem(me + blocks - 1, blocks), dp_count, sp_count)

    def load(source, which, head):
        columns = pl.ds(head * HEAD_SIZE, HEAD_SIZE)
        return pltpu.make_async_copy(
            source.at[:, columns], held.at[0, head, which], kv_sem.at[head, which]
        )

    def load_q(head):
        columns = pl.ds(head * width, width)
        return pltpu.make_async_copy(q_hbm.at[:, columns], q_buf.at[:, columns], q_sem.at[head])

    def send(hop, head):
        return pltpu.make_async_remote_copy(
            src_ref=held.at[hop, head],
            dst_ref=held.at[hop + 1, head],
            send_sem=send_sem.at[hop, head],
            recv_sem=recv_sem.at[hop, head],
            device_id=right,
            device_id_type=MESH,
        )

    ahead = sp_count - position
    crosses = (ahead <= hops) & (me + ahead < blocks)
    across = place(jnp.minimum(me + ahead, blocks - 1), dp_count, sp_count)
    edge = (dp == dp_count - 1) & (ahead <= hops)
    lends = edge & (tp == tp_count - 2)
    carries = edge & (tp == tp_count - 1) & (tp_count > 1)
    own = heads - heads // 2
    carrier = {"tp": jnp.minimum(tp + 1, tp_count - 1), "dp": dp, "sp": position}
    lender = {"tp": jnp.maximum(tp - 1, 0), "dp": dp, "sp": position}
    goal = {"tp": tp, "dp": 0, "sp": 0}

    def sends(hop):
        return (me >= hop) & (position < sp_count - 1)

    def start_send(hop, head):
        @pl.when(sends(hop))
        def _():
            send(hop, head).start()

    def wait_receive(hop, head):
        @pl.when(me >= hop)
        def _():
            send(hop - 1, head).wait_recv()

    def send_across(source, sem, target, distance, head):
        return pltpu.make_async_remote_copy(
            src_ref=source,
            dst_ref=held.at[distance, head],
            send_sem=sem.at[head],
            recv_sem=recv_sem.at[distance - 1, head],
            device_id=target,
            device_id_type=MESH,
        )

    def lend(head):
        return pltpu.make_async_remote_copy(
            src_ref=held.at[0, head],
            dst_ref=carried.at[head - own],
            send_sem=across_sem.at[head],
            recv_sem=lent_sem.at[head],
            device_id=carrier,
            device_id_type=MESH,
        )

    def each_lent(action):
        @pl.when(lends)
        def _():
            for head in range(own, heads):
                action(lend(head))

    def each_across(action):
        for distance in range(1, hops + 1):

            @pl.when(crosses & (ahead == distance))
            def _():
                for head in range(own):
                    action(send_across(held.at[0, head], across_sem, across, distance, head))

                @pl.when(jnp.logical_not(lends))
                def _():
                    for head in range(own, heads):
                        action(send_across(held.at[0, head], across_sem, across, distance, head))

    def each_carried(action):
        for distance in range(1, hops + 1):

            @pl.when(carries & (ahead == distance))
            def _():
                for head in range(own, heads):
                    action(head, send_across(carried.at[head - own], carried_sem, goal, distance, head))

    def forward(head, copy):
        lend(head).wait_recv()
        copy.start()

    get_lengths = pltpu.make_async_copy(lengths_hbm, lengths, lengths_sem)
    for head in range(heads):
        load(k_hbm, 0, head).start()
        load(v_hbm, 1, head).start()
    for head in range(heads):
        load_q(head).start()
    get_lengths.start()

    barrier = pltpu.get_barrier_semaphore()

    def greet(device):
        pl.semaphore_signal(barrier, inc=1, device_id=device, device_id_type=MESH)

    @pl.when(position > 0)
    def _():
        greet(left)

    for distance in range(1, hops + 1):

        @pl.when((position == 0) & (me >= distance))
        def _():
            greet(place(jnp.maximum(me - distance, 0), dp_count, sp_count))

        @pl.when((position == 0) & (dp == 0) & (tp == tp_count - 1) & (tp_count > 1))
        def _():
            greet({"tp": tp, "dp": dp_count - 1, "sp": sp_count - distance})

    @pl.when(carries)
    def _():
        greet(lender)

    peers = [position < sp_count - 1, crosses, lends, carries]
    count = sum(peer.astype(jnp.int32) for peer in peers)
    for number in range(1, len(peers) + 1):

        @pl.when(count == number)
        def _():
            pl.semaphore_wait(barrier, number)

    for head in range(heads):
        load(k_hbm, 0, head).wait()
        load(v_hbm, 1, head).wait()
        start_send(0, head)
    each_lent(lambda copy: copy.start())
    each_across(lambda copy: copy.start())
    each_carried(forward)
    for hop in range(1, hops + 1):

        @pl.when(me < hop)
        def _():
            held[hop] = jnp.zeros_like(held[hop])

    get_lengths.wait()
    base = me * rows
    row = lax.broadcasted_iota(jnp.int32, (rows, rows), 0)
    column = lax.broadcasted_iota(jnp.int32, (rows, rows), 1)
    near = column <= row
    first = jnp.zeros((rows, rows), jnp.int32)
    end = jnp.int32(0)
    for entry in range(lengths.shape[0]):
        end = end + lengths[entry]
        first = jnp.where(base + row >= end, end, first)
    mixed_position = base + column - jnp.where(near, 0, hops * rows)
    bias[0] = jnp.where(mixed_position >= first, 0.0, DEAD)
    for hop in range(1, hops):
        bias[hop] = jnp.where(base - hop * rows + column >= first, 0.0, DEAD)

    for hop in range(1, hops):
        for head in range(heads):
            wait_receive(hop, head)
            start_send(hop, head)

    factor = HEAD_SIZE ** (-0.5) * math.log2(math.e)
    span = (hops + 1) * rows
    batch = math.gcd(group, 8)
    for head in range(heads):
        wait_receive(hops, head)
        load_q(head).wait()
        k_all = held[:, head, 0].reshape(span, HEAD_SIZE)
        v_all = held[:, head, 1].reshape(span, HEAD_SIZE)
        for member in range(0, group, batch):
            at = [head * width + (member + other) * HEAD_SIZE for other in range(batch)]
            q_rows = jnp.concatenate([q_buf[:, a : a + HEAD_SIZE] for a in at], axis=0)
            score = lax.dot_general(
                q_rows, k_all, (((1,), (1,)), ((), ())), preferred_element_type=jnp.float32
            ).reshape(batch, rows, span)
            parts = [score[:, :, hop * rows : (hop + 1) * rows] for hop in range(hops + 1)]
            mixed = jnp.where(near, parts[0], parts[hops])
            parts = [part + bias[hop] for hop, part in enumerate([mixed] + parts[1:hops])]
            top = jnp.max(functools.reduce(jnp.maximum, parts), axis=2, keepdims=True)
            weights = [jnp.exp2((part - top) * factor) for part in parts]
            total = jnp.sum(sum(weights[1:], weights[0]), axis=2, keepdims=True)
            ends = [jnp.where(near, weights[0], 0.0), jnp.where(near, 0.0, weights[0])]
            weight = jnp.concatenate([ends[0]] + weights[1:] + [ends[1]], axis=2)
            weight = weight.astype(jnp.bfloat16).reshape(batch * rows, span)
            summed = jnp.dot(weight, v_all, preferred_element_type=jnp.float32)
            result = (summed.reshape(batch, rows, HEAD_SIZE) / total).astype(jnp.bfloat16)
            for other, a in enumerate(at):
                out_buf[:, a : a + HEAD_SIZE] = result[other]

    for hop in range(hops):
        for head in range(heads):

            @pl.when(sends(hop))
            def _():
                send(hop, head).wait_send()
    each_lent(lambda copy: copy.wait_send())
    each_across(lambda copy: copy.wait_send())
    each_carried(lambda head, copy: copy.wait_send())


def solution(mesh):
    tp_count, dp_count, sp_count = (mesh.shape[axis] for axis in ("tp", "dp", "sp"))
    hops = max(sp_count // 2, 1)

    def local(queries, keys, values, doc_lengths):
        rows, width = queries.shape
        heads = keys.shape[1] // HEAD_SIZE
        group = width // keys.shape[1]
        sizes = (tp_count, dp_count, sp_count, hops, heads, group)
        hbm = pl.BlockSpec(memory_space=pltpu.HBM)
        return pl.pallas_call(
            functools.partial(kernel, sizes),
            out_shape=pltpu.VMEM((rows, width), jnp.bfloat16),
            in_specs=[hbm, hbm, hbm, hbm],
            out_specs=pl.BlockSpec(memory_space=pltpu.VMEM),
            scratch_shapes=[
                pltpu.VMEM((rows, width), jnp.bfloat16),
                pltpu.VMEM((hops + 1, heads, 2, rows, HEAD_SIZE), jnp.bfloat16),
                pltpu.VMEM((hops, rows, rows), jnp.float32),
                pltpu.SMEM(doc_lengths.shape, jnp.int32),
                pltpu.SemaphoreType.DMA((heads,)),
                pltpu.SemaphoreType.DMA((heads, 2)),
                pltpu.SemaphoreType.DMA((hops, heads)),
                pltpu.SemaphoreType.DMA((hops, heads)),
                pltpu.SemaphoreType.DMA,
                pltpu.SemaphoreType.DMA((heads,)),
                pltpu.VMEM((max(heads // 2, 1), 2, rows, HEAD_SIZE), jnp.bfloat16),
                pltpu.SemaphoreType.DMA((heads,)),
                pltpu.SemaphoreType.DMA((heads,)),
            ],
            compiler_params=pltpu.CompilerParams(collective_id=0, has_side_effects=True, vmem_limit_bytes=32 << 20),
        )(*(pltpu.with_memory_space_constraint(a, pltpu.HBM) for a in (queries, keys, values, doc_lengths)))

    spec = P(("groups", "tp", "dp", "sp"), None)
    return jax.shard_map(
        local, mesh=mesh, in_specs=(spec, spec, spec, P("groups")), out_specs=spec, check_vma=False
    )
```

```python
import functools
import math

import jax
import jax.numpy as jnp
from jax import lax
from jax.experimental import pallas as pl
from jax.experimental.pallas import tpu as pltpu
from jax.sharding import PartitionSpec as P

HEAD_SIZE = 128
MESH = pl.DeviceIdType.MESH
DEAD = -1e30


def place(index, dp_count, sp_count):
    return {
        "tp": index // (dp_count * sp_count),
        "dp": (index // sp_count) % dp_count,
        "sp": index % sp_count,
    }


def attend(rows, hops, near, bias, keys, values, q_refs, out_refs):
    factor = HEAD_SIZE ** (-0.5) * math.log2(math.e)
    span = (hops + 1) * rows
    count = len(q_refs)
    q_rows = jnp.concatenate([ref[...] for ref in q_refs], axis=0)
    score = lax.dot_general(
        q_rows, keys.reshape(span, HEAD_SIZE), (((1,), (1,)), ((), ())),
        preferred_element_type=jnp.float32,
    ).reshape(count, rows, span)
    parts = [score[:, :, hop * rows : (hop + 1) * rows] for hop in range(hops + 1)]
    mixed = jnp.where(near, parts[0], parts[hops])
    parts = [part + bias[hop] for hop, part in enumerate([mixed] + parts[1:hops])]
    top = jnp.max(functools.reduce(jnp.maximum, parts), axis=2, keepdims=True)
    weights = [jnp.exp2((part - top) * factor) for part in parts]
    total = jnp.sum(sum(weights[1:], weights[0]), axis=2, keepdims=True)
    ends = [jnp.where(near, weights[0], 0.0), jnp.where(near, 0.0, weights[0])]
    weight = jnp.concatenate([ends[0]] + weights[1:] + [ends[1]], axis=2)
    weight = weight.astype(jnp.bfloat16).reshape(count * rows, span)
    summed = jnp.dot(weight, values.reshape(span, HEAD_SIZE), preferred_element_type=jnp.float32)
    result = (summed.reshape(count, rows, HEAD_SIZE) / total).astype(jnp.bfloat16)
    for member, ref in enumerate(out_refs):
        ref[...] = result[member]


def finish(hops, group, part, last_kv, last_q, bias, out_hbm, buffer, sems):
    rows, width = part.shape[0], group * HEAD_SIZE
    done = part.shape[1] - width
    columns = pl.ds(0, done)
    early = pltpu.make_async_copy(part.at[:, columns], out_hbm.at[:, columns], sems.at[0])
    if done:
        early.start()
    row = lax.broadcasted_iota(jnp.int32, (rows, rows), 0)
    near = lax.broadcasted_iota(jnp.int32, (rows, rows), 1) <= row
    at = [pl.ds(member * HEAD_SIZE, HEAD_SIZE) for member in range(group)]
    attend(
        rows, hops, near, bias, last_kv[:, 0], last_kv[:, 1],
        [last_q.at[:, a] for a in at], [buffer.at[:, a] for a in at],
    )
    late = pltpu.make_async_copy(buffer, out_hbm.at[:, pl.ds(done, width)], sems.at[1])
    late.start()
    if done:
        early.wait()
    late.wait()


def kernel(
    sizes, q_hbm, k_hbm, v_hbm, lengths_hbm, out_buf, last_kv, last_q, bias,
    q_buf, held, lengths, q_sem, kv_sem, send_sem, recv_sem, lengths_sem, across_sem, carried, lent_sem, carried_sem,
):
    tp_count, dp_count, sp_count, hops, heads, group = sizes
    rows = q_hbm.shape[0]
    width = group * HEAD_SIZE
    blocks = tp_count * dp_count * sp_count
    tp, dp, position = (lax.axis_index(axis) for axis in ("tp", "dp", "sp"))
    me = (tp * dp_count + dp) * sp_count + position
    right = place(lax.rem(me + 1, blocks), dp_count, sp_count)
    left = place(lax.rem(me + blocks - 1, blocks), dp_count, sp_count)

    def load(source, which, head):
        columns = pl.ds(head * HEAD_SIZE, HEAD_SIZE)
        return pltpu.make_async_copy(
            source.at[:, columns], held.at[0, head, which], kv_sem.at[head, which]
        )

    def load_q(head):
        columns = pl.ds(head * width, width)
        target = last_q if head == heads - 1 else q_buf.at[:, columns]
        return pltpu.make_async_copy(q_hbm.at[:, columns], target, q_sem.at[head])

    def send(hop, head):
        return pltpu.make_async_remote_copy(
            src_ref=held.at[hop, head],
            dst_ref=held.at[hop + 1, head],
            send_sem=send_sem.at[hop, head],
            recv_sem=recv_sem.at[hop, head],
            device_id=right,
            device_id_type=MESH,
        )

    ahead = sp_count - position
    crosses = (ahead <= hops) & (me + ahead < blocks)
    across = place(jnp.minimum(me + ahead, blocks - 1), dp_count, sp_count)
    edge = (dp == dp_count - 1) & (ahead <= hops)
    lends = edge & (tp == tp_count - 2)
    carries = edge & (tp == tp_count - 1) & (tp_count > 1)
    own = heads - heads // 2
    carrier = {"tp": jnp.minimum(tp + 1, tp_count - 1), "dp": dp, "sp": position}
    lender = {"tp": jnp.maximum(tp - 1, 0), "dp": dp, "sp": position}
    goal = {"tp": tp, "dp": 0, "sp": 0}

    def sends(hop):
        return (me >= hop) & (position < sp_count - 1)

    def start_send(hop, head):
        @pl.when(sends(hop))
        def _():
            send(hop, head).start()

    def wait_receive(hop, head):
        @pl.when(me >= hop)
        def _():
            send(hop - 1, head).wait_recv()

    def send_across(source, sem, target, distance, head):
        return pltpu.make_async_remote_copy(
            src_ref=source,
            dst_ref=held.at[distance, head],
            send_sem=sem.at[head],
            recv_sem=recv_sem.at[distance - 1, head],
            device_id=target,
            device_id_type=MESH,
        )

    def lend(head):
        return pltpu.make_async_remote_copy(
            src_ref=held.at[0, head],
            dst_ref=carried.at[head - own],
            send_sem=across_sem.at[head],
            recv_sem=lent_sem.at[head],
            device_id=carrier,
            device_id_type=MESH,
        )

    def each_lent(action):
        @pl.when(lends)
        def _():
            for head in range(own, heads):
                action(lend(head))

    def each_across(action):
        for distance in range(1, hops + 1):

            @pl.when(crosses & (ahead == distance))
            def _():
                for head in range(own):
                    action(send_across(held.at[0, head], across_sem, across, distance, head))

                @pl.when(jnp.logical_not(lends))
                def _():
                    for head in range(own, heads):
                        action(send_across(held.at[0, head], across_sem, across, distance, head))

    def each_carried(action):
        for distance in range(1, hops + 1):

            @pl.when(carries & (ahead == distance))
            def _():
                for head in range(own, heads):
                    action(head, send_across(carried.at[head - own], carried_sem, goal, distance, head))

    def forward(head, copy):
        lend(head).wait_recv()
        copy.start()

    get_lengths = pltpu.make_async_copy(lengths_hbm, lengths, lengths_sem)
    for head in range(heads):
        load(k_hbm, 0, head).start()
        load(v_hbm, 1, head).start()
    for head in range(heads):
        load_q(head).start()
    get_lengths.start()

    barrier = pltpu.get_barrier_semaphore()

    def greet(device):
        pl.semaphore_signal(barrier, inc=1, device_id=device, device_id_type=MESH)

    @pl.when(position > 0)
    def _():
        greet(left)

    for distance in range(1, hops + 1):

        @pl.when((position == 0) & (me >= distance))
        def _():
            greet(place(jnp.maximum(me - distance, 0), dp_count, sp_count))

        @pl.when((position == 0) & (dp == 0) & (tp == tp_count - 1) & (tp_count > 1))
        def _():
            greet({"tp": tp, "dp": dp_count - 1, "sp": sp_count - distance})

    @pl.when(carries)
    def _():
        greet(lender)

    peers = [position < sp_count - 1, crosses, lends, carries]
    count = sum(peer.astype(jnp.int32) for peer in peers)
    for number in range(1, len(peers) + 1):

        @pl.when(count == number)
        def _():
            pl.semaphore_wait(barrier, number)

    for head in range(heads):
        load(k_hbm, 0, head).wait()
        load(v_hbm, 1, head).wait()
        start_send(0, head)
    each_lent(lambda copy: copy.start())
    each_across(lambda copy: copy.start())
    each_carried(forward)
    for hop in range(1, hops + 1):

        @pl.when(me < hop)
        def _():
            held[hop] = jnp.zeros_like(held[hop])

    get_lengths.wait()
    base = me * rows
    row = lax.broadcasted_iota(jnp.int32, (rows, rows), 0)
    column = lax.broadcasted_iota(jnp.int32, (rows, rows), 1)
    near = column <= row
    first = jnp.zeros((rows, rows), jnp.int32)
    end = jnp.int32(0)
    for entry in range(lengths.shape[0]):
        end = end + lengths[entry]
        first = jnp.where(base + row >= end, end, first)
    mixed_position = base + column - jnp.where(near, 0, hops * rows)
    bias[0] = jnp.where(mixed_position >= first, 0.0, DEAD)
    for hop in range(1, hops):
        bias[hop] = jnp.where(base - hop * rows + column >= first, 0.0, DEAD)

    for hop in range(1, hops):
        for head in range(heads):
            wait_receive(hop, head)
            start_send(hop, head)

    for head in range(heads - 1):
        wait_receive(hops, head)
        load_q(head).wait()
        at = [head * width + member * HEAD_SIZE for member in range(group)]
        attend(
            rows, hops, near, bias, held[:, head, 0], held[:, head, 1],
            [q_buf.at[:, pl.ds(a, HEAD_SIZE)] for a in at],
            [out_buf.at[:, pl.ds(a, HEAD_SIZE)] for a in at],
        )
    load_q(heads - 1).wait()
    wait_receive(hops, heads - 1)
    last_kv[...] = held[:, heads - 1]

    for hop in range(hops):
        for head in range(heads):

            @pl.when(sends(hop))
            def _():
                send(hop, head).wait_send()
    each_lent(lambda copy: copy.wait_send())
    each_across(lambda copy: copy.wait_send())
    each_carried(lambda head, copy: copy.wait_send())


def solution(mesh):
    tp_count, dp_count, sp_count = (mesh.shape[axis] for axis in ("tp", "dp", "sp"))
    hops = max(sp_count // 2, 1)

    def local(queries, keys, values, doc_lengths):
        rows, width = queries.shape
        heads = keys.shape[1] // HEAD_SIZE
        group = width // keys.shape[1]
        sizes = (tp_count, dp_count, sp_count, hops, heads, group)
        hbm = pl.BlockSpec(memory_space=pltpu.HBM)
        vmem = pl.BlockSpec(memory_space=pltpu.VMEM)
        results = pl.pallas_call(
            functools.partial(kernel, sizes),
            out_shape=(
                pltpu.VMEM((rows, width), jnp.bfloat16),
                pltpu.VMEM((hops + 1, 2, rows, HEAD_SIZE), jnp.bfloat16),
                pltpu.VMEM((rows, group * HEAD_SIZE), jnp.bfloat16),
                pltpu.VMEM((hops, rows, rows), jnp.float32),
            ),
            in_specs=[hbm, hbm, hbm, hbm],
            out_specs=(vmem,) * 4,
            scratch_shapes=[
                pltpu.VMEM((rows, width), jnp.bfloat16),
                pltpu.VMEM((hops + 1, heads, 2, rows, HEAD_SIZE), jnp.bfloat16),
                pltpu.SMEM(doc_lengths.shape, jnp.int32),
                pltpu.SemaphoreType.DMA((heads,)),
                pltpu.SemaphoreType.DMA((heads, 2)),
                pltpu.SemaphoreType.DMA((hops, heads)),
                pltpu.SemaphoreType.DMA((hops, heads)),
                pltpu.SemaphoreType.DMA,
                pltpu.SemaphoreType.DMA((heads,)),
                pltpu.VMEM((max(heads // 2, 1), 2, rows, HEAD_SIZE), jnp.bfloat16),
                pltpu.SemaphoreType.DMA((heads,)),
                pltpu.SemaphoreType.DMA((heads,)),
            ],
            compiler_params=pltpu.CompilerParams(collective_id=0, has_side_effects=True, vmem_limit_bytes=32 << 20),
        )(*(pltpu.with_memory_space_constraint(a, pltpu.HBM) for a in (queries, keys, values, doc_lengths)))
        return pl.pallas_call(
            functools.partial(finish, hops, group),
            out_shape=jax.ShapeDtypeStruct((rows, width), jnp.bfloat16),
            in_specs=[vmem] * 4,
            out_specs=hbm,
            scratch_shapes=[
                pltpu.VMEM((rows, group * HEAD_SIZE), jnp.bfloat16),
                pltpu.SemaphoreType.DMA((2,)),
            ],
            compiler_params=pltpu.CompilerParams(vmem_limit_bytes=32 << 20),
        )(*(pltpu.with_memory_space_constraint(a, pltpu.VMEM) for a in results))

    spec = P(("groups", "tp", "dp", "sp"), None)
    return jax.shard_map(
        local, mesh=mesh, in_specs=(spec, spec, spec, P("groups")), out_specs=spec, check_vma=False
    )
```

```python
import functools
import math

import jax
import jax.numpy as jnp
from jax import lax
from jax.experimental import pallas as pl
from jax.experimental.pallas import tpu as pltpu
from jax.sharding import PartitionSpec as P

HEAD_SIZE = 128
MESH = pl.DeviceIdType.MESH
DEAD = -1e30


def place(index, dp_count, sp_count):
    return {
        "tp": index // (dp_count * sp_count),
        "dp": (index // sp_count) % dp_count,
        "sp": index % sp_count,
    }


def attend(rows, hops, near, bias, keys, values, q_refs, out_refs):
    factor = HEAD_SIZE ** (-0.5) * math.log2(math.e)
    span = (hops + 1) * rows
    count = len(q_refs)
    q_rows = jnp.concatenate([ref[...] for ref in q_refs], axis=0)
    score = lax.dot_general(
        q_rows, keys.reshape(span, HEAD_SIZE), (((1,), (1,)), ((), ())),
        preferred_element_type=jnp.float32,
    ).reshape(count, rows, span)
    parts = [score[:, :, hop * rows : (hop + 1) * rows] for hop in range(hops + 1)]
    mixed = jnp.where(near, parts[0], parts[hops])
    parts = [part + bias[hop] for hop, part in enumerate([mixed] + parts[1:hops])]
    top = jnp.max(functools.reduce(jnp.maximum, parts), axis=2, keepdims=True)
    weights = [jnp.exp2((part - top) * factor) for part in parts]
    total = jnp.sum(sum(weights[1:], weights[0]), axis=2, keepdims=True)
    ends = [jnp.where(near, weights[0], 0.0), jnp.where(near, 0.0, weights[0])]
    weight = jnp.concatenate([ends[0]] + weights[1:] + [ends[1]], axis=2)
    weight = weight.astype(jnp.bfloat16).reshape(count * rows, span)
    summed = jnp.dot(weight, values.reshape(span, HEAD_SIZE), preferred_element_type=jnp.float32)
    result = (summed.reshape(count, rows, HEAD_SIZE) / total).astype(jnp.bfloat16)
    for member, ref in enumerate(out_refs):
        ref[...] = result[member]


def finish(hops, group, part, last_kv, last_q, bias, out_hbm, buffer, sems):
    rows, width = part.shape[0], group * HEAD_SIZE
    done = part.shape[1] - width
    columns = pl.ds(0, done)
    early = pltpu.make_async_copy(part.at[:, columns], out_hbm.at[:, columns], sems.at[0])
    if done:
        early.start()
    row = lax.broadcasted_iota(jnp.int32, (rows, rows), 0)
    near = lax.broadcasted_iota(jnp.int32, (rows, rows), 1) <= row
    at = [pl.ds(member * HEAD_SIZE, HEAD_SIZE) for member in range(group)]
    attend(
        rows, hops, near, bias, last_kv[:, 0], last_kv[:, 1],
        [last_q.at[:, a] for a in at], [buffer.at[:, a] for a in at],
    )
    late = pltpu.make_async_copy(buffer, out_hbm.at[:, pl.ds(done, width)], sems.at[1])
    late.start()
    if done:
        early.wait()
    late.wait()


def kernel(
    sizes, q_hbm, k_hbm, v_hbm, lengths_hbm, out_buf, last_kv, last_q, bias,
    q_buf, held, lengths, q_sem, kv_sem, send_sem, recv_sem, lengths_sem, across_sem, carried, lent_sem, carried_sem,
):
    tp_count, dp_count, sp_count, hops, heads, group = sizes
    rows = q_hbm.shape[0]
    width = group * HEAD_SIZE
    blocks = tp_count * dp_count * sp_count
    tp, dp, position = (lax.axis_index(axis) for axis in ("tp", "dp", "sp"))
    me = (tp * dp_count + dp) * sp_count + position
    right = place(lax.rem(me + 1, blocks), dp_count, sp_count)
    left = place(lax.rem(me + blocks - 1, blocks), dp_count, sp_count)

    def load(source, which, head):
        columns = pl.ds(head * HEAD_SIZE, HEAD_SIZE)
        return pltpu.make_async_copy(
            source.at[:, columns], held.at[0, head, which], kv_sem.at[head, which]
        )

    def load_q(head):
        columns = pl.ds(head * width, width)
        target = last_q if head == heads - 1 else q_buf.at[:, columns]
        return pltpu.make_async_copy(q_hbm.at[:, columns], target, q_sem.at[head])

    def send(hop, head):
        return pltpu.make_async_remote_copy(
            src_ref=held.at[hop, head],
            dst_ref=held.at[hop + 1, head],
            send_sem=send_sem.at[hop, head],
            recv_sem=recv_sem.at[hop, head],
            device_id=right,
            device_id_type=MESH,
        )

    ahead = sp_count - position
    crosses = (ahead <= hops) & (me + ahead < blocks)
    across = place(jnp.minimum(me + ahead, blocks - 1), dp_count, sp_count)
    edge = (dp == dp_count - 1) & (ahead <= hops)
    lends = edge & (tp == tp_count - 2)
    carries = edge & (tp == tp_count - 1) & (tp_count > 1)
    own = heads - heads // 2
    carrier = {"tp": jnp.minimum(tp + 1, tp_count - 1), "dp": dp, "sp": position}
    lender = {"tp": jnp.maximum(tp - 1, 0), "dp": dp, "sp": position}
    goal = {"tp": tp, "dp": 0, "sp": 0}

    def sends(hop):
        return (me >= hop) & (position < sp_count - 1)

    def start_send(hop, head):
        @pl.when(sends(hop))
        def _():
            send(hop, head).start()

    def wait_receive(hop, head):
        @pl.when(me >= hop)
        def _():
            send(hop - 1, head).wait_recv()

    def send_across(source, sem, target, distance, head):
        return pltpu.make_async_remote_copy(
            src_ref=source,
            dst_ref=held.at[distance, head],
            send_sem=sem.at[head],
            recv_sem=recv_sem.at[distance - 1, head],
            device_id=target,
            device_id_type=MESH,
        )

    def lend(head):
        return pltpu.make_async_remote_copy(
            src_ref=held.at[0, head],
            dst_ref=carried.at[head - own],
            send_sem=across_sem.at[head],
            recv_sem=lent_sem.at[head],
            device_id=carrier,
            device_id_type=MESH,
        )

    def each_lent(action):
        @pl.when(lends)
        def _():
            for head in range(own, heads):
                action(lend(head))

    def each_across(action):
        for distance in range(1, hops + 1):

            @pl.when(crosses & (ahead == distance))
            def _():
                for head in range(own):
                    action(send_across(held.at[0, head], across_sem, across, distance, head))

                @pl.when(jnp.logical_not(lends))
                def _():
                    for head in range(own, heads):
                        action(send_across(held.at[0, head], across_sem, across, distance, head))

    def each_carried(action):
        for distance in range(1, hops + 1):

            @pl.when(carries & (ahead == distance))
            def _():
                for head in range(own, heads):
                    action(head, send_across(carried.at[head - own], carried_sem, goal, distance, head))

    def forward(head, copy):
        lend(head).wait_recv()
        copy.start()

    get_lengths = pltpu.make_async_copy(lengths_hbm, lengths, lengths_sem)
    barrier = pltpu.get_barrier_semaphore()

    def greet(device):
        pl.semaphore_signal(barrier, inc=1, device_id=device, device_id_type=MESH)

    @pl.when(position > 0)
    def _():
        greet(left)

    for distance in range(1, hops + 1):

        @pl.when((position == 0) & (me >= distance))
        def _():
            greet(place(jnp.maximum(me - distance, 0), dp_count, sp_count))

        @pl.when((position == 0) & (dp == 0) & (tp == tp_count - 1) & (tp_count > 1))
        def _():
            greet({"tp": tp, "dp": dp_count - 1, "sp": sp_count - distance})

    @pl.when(carries)
    def _():
        greet(lender)

    for head in range(heads):
        load(k_hbm, 0, head).start()
        load(v_hbm, 1, head).start()
    for head in range(heads):
        load_q(head).start()
    get_lengths.start()

    peers = [position < sp_count - 1, crosses, lends, carries]
    count = sum(peer.astype(jnp.int32) for peer in peers)
    for number in range(1, len(peers) + 1):

        @pl.when(count == number)
        def _():
            pl.semaphore_wait(barrier, number)

    for head in range(heads):
        load(k_hbm, 0, head).wait()
        load(v_hbm, 1, head).wait()
        start_send(0, head)
    each_lent(lambda copy: copy.start())
    each_across(lambda copy: copy.start())
    each_carried(forward)
    for hop in range(1, hops + 1):

        @pl.when(me < hop)
        def _():
            held[hop] = jnp.zeros_like(held[hop])

    get_lengths.wait()
    base = me * rows
    row = lax.broadcasted_iota(jnp.int32, (rows, rows), 0)
    column = lax.broadcasted_iota(jnp.int32, (rows, rows), 1)
    near = column <= row
    first = jnp.zeros((rows, rows), jnp.int32)
    end = jnp.int32(0)
    for entry in range(lengths.shape[0]):
        end = end + lengths[entry]
        first = jnp.where(base + row >= end, end, first)
    mixed_position = base + column - jnp.where(near, 0, hops * rows)
    bias[0] = jnp.where(mixed_position >= first, 0.0, DEAD)
    for hop in range(1, hops):
        bias[hop] = jnp.where(base - hop * rows + column >= first, 0.0, DEAD)

    for hop in range(1, hops):
        for head in range(heads):
            wait_receive(hop, head)
            start_send(hop, head)

    for head in range(heads - 1):
        wait_receive(hops, head)
        load_q(head).wait()
        at = [head * width + member * HEAD_SIZE for member in range(group)]
        attend(
            rows, hops, near, bias, held[:, head, 0], held[:, head, 1],
            [q_buf.at[:, pl.ds(a, HEAD_SIZE)] for a in at],
            [out_buf.at[:, pl.ds(a, HEAD_SIZE)] for a in at],
        )
    load_q(heads - 1).wait()
    last_kv[:hops] = held[:hops, heads - 1]
    wait_receive(hops, heads - 1)
    last_kv[hops] = held[hops, heads - 1]

    for hop in range(hops):
        for head in range(heads):

            @pl.when(sends(hop))
            def _():
                send(hop, head).wait_send()
    each_lent(lambda copy: copy.wait_send())
    each_across(lambda copy: copy.wait_send())
    each_carried(lambda head, copy: copy.wait_send())


def solution(mesh):
    tp_count, dp_count, sp_count = (mesh.shape[axis] for axis in ("tp", "dp", "sp"))
    hops = max(sp_count // 2, 1)

    def local(queries, keys, values, doc_lengths):
        rows, width = queries.shape
        heads = keys.shape[1] // HEAD_SIZE
        group = width // keys.shape[1]
        sizes = (tp_count, dp_count, sp_count, hops, heads, group)
        hbm = pl.BlockSpec(memory_space=pltpu.HBM)
        vmem = pl.BlockSpec(memory_space=pltpu.VMEM)
        results = pl.pallas_call(
            functools.partial(kernel, sizes),
            out_shape=(
                pltpu.VMEM((rows, width), jnp.bfloat16),
                pltpu.VMEM((hops + 1, 2, rows, HEAD_SIZE), jnp.bfloat16),
                pltpu.VMEM((rows, group * HEAD_SIZE), jnp.bfloat16),
                pltpu.VMEM((hops, rows, rows), jnp.float32),
            ),
            in_specs=[hbm, hbm, hbm, hbm],
            out_specs=(vmem,) * 4,
            scratch_shapes=[
                pltpu.VMEM((rows, width), jnp.bfloat16),
                pltpu.VMEM((hops + 1, heads, 2, rows, HEAD_SIZE), jnp.bfloat16),
                pltpu.SMEM(doc_lengths.shape, jnp.int32),
                pltpu.SemaphoreType.DMA((heads,)),
                pltpu.SemaphoreType.DMA((heads, 2)),
                pltpu.SemaphoreType.DMA((hops, heads)),
                pltpu.SemaphoreType.DMA((hops, heads)),
                pltpu.SemaphoreType.DMA,
                pltpu.SemaphoreType.DMA((heads,)),
                pltpu.VMEM((max(heads // 2, 1), 2, rows, HEAD_SIZE), jnp.bfloat16),
                pltpu.SemaphoreType.DMA((heads,)),
                pltpu.SemaphoreType.DMA((heads,)),
            ],
            compiler_params=pltpu.CompilerParams(collective_id=0, has_side_effects=True, vmem_limit_bytes=32 << 20),
        )(*(pltpu.with_memory_space_constraint(a, pltpu.HBM) for a in (queries, keys, values, doc_lengths)))
        return pl.pallas_call(
            functools.partial(finish, hops, group),
            out_shape=jax.ShapeDtypeStruct((rows, width), jnp.bfloat16),
            in_specs=[vmem] * 4,
            out_specs=hbm,
            scratch_shapes=[
                pltpu.VMEM((rows, group * HEAD_SIZE), jnp.bfloat16),
                pltpu.SemaphoreType.DMA((2,)),
            ],
            compiler_params=pltpu.CompilerParams(vmem_limit_bytes=32 << 20),
        )(*(pltpu.with_memory_space_constraint(a, pltpu.VMEM) for a in results))

    spec = P(("groups", "tp", "dp", "sp"), None)
    return jax.shard_map(
        local, mesh=mesh, in_specs=(spec, spec, spec, P("groups")), out_specs=spec, check_vma=False
    )
```
